1024 devices in a mesh: replica: 64 (over y, z_lo, core), fsdp: 16 (over z_hi, x).
Axes of the slice: x: 4, y: 4, z: 32 (z_hi: 4, z_lo: 8; z = z_hi * 8 + z_lo), core: 2. Of those that a mesh axis runs over, the one named last changes fastest.
Arguments:
- local_weight: bfloat16 [64, 512, 8192], P('replica', None, 'fsdp'), may hold values from -0.75 to 0.75
- anchor: float32 [512, 8192], P(None, 'fsdp'), may hold values from -0.25 to 0.25
- momentum: float32 [512, 8192], P('replica', 'fsdp'), may hold values from -0.3 to 0.3
- tokens: bfloat16 [131072, 512], P(('replica', 'fsdp')), may hold values from -6 to 6
Outputs:
- blended_weight: bfloat16 [64, 512, 8192], P('replica', None, 'fsdp')
- anchor_out: float32 [512, 8192], P(None, 'fsdp')
- momentum_out: float32 [512, 8192], P('replica', 'fsdp')
- product_out: bfloat16 [131072, 8192], P(('replica', 'fsdp'))
The draws below stay inside these ranges and needn't reach their ends.
All inputs are finite; a program needn't handle non-finite values.
Results may differ from the reference program's by a relative error of at most 0.0051.
Values may be sent and summed in bfloat16 or wider, within the bound.
No kernel may reach another device: no remote copies, remote signals or barrier semaphores. Data moves between devices by JAX's collectives and lax.ppermute only.
A program may use at most 32 MiB of HBM per device.

```python
import jax
import jax.numpy as jnp
from jax import lax

D = 8192
FRAG = 512
WORKERS = 64
TOKENS = 131072


def spiked(result, rng, source, target, shards_of, factor):
    owner, partner = [(jnp.arange(result.shape[axis_at]) // (result.shape[axis_at] // shards_of)).reshape([-1 if axis == axis_at else 1 for axis in range(result.ndim)]) for axis_at in (source, target)]
    chosen = jax.random.permutation(rng, shards_of)[partner]
    strong = (owner == chosen) | (owner == (partner + shards_of // 2) % shards_of)
    return jnp.where(strong, factor * result, result)


def shard_levels(key, extent, cuts, least, high):
    gain = 1.0
    for position, blocks in cuts:
        steps = jax.random.uniform(jax.random.fold_in(jax.random.fold_in(key, 6), position), (blocks,), jnp.float32, least / len(cuts), high / len(cuts))
        gain = gain * jnp.repeat(jnp.exp(steps), extent[position] // blocks).reshape((-1,) + (1,) * (len(extent) - 1 - position))
    return gain


def bell_draw(stream_key, shape, scale, reach, split=(), dtype=jnp.bfloat16):
    values = scale * jax.random.normal(stream_key, shape, jnp.float32)
    if split:
        values = values * shard_levels(stream_key, shape, split, -0.22, 0.18)
    return jnp.clip(values, -reach, reach).astype(dtype)


def bell_draw_with(stream_key, dims, deviation, limit, split, heavy, kind=jnp.bfloat16):
    array = deviation * jax.random.normal(stream_key, dims, jnp.float32)
    if split:
        array = array * shard_levels(stream_key, dims, split, -0.22, 0.18)
    return jnp.clip(spiked(array, jax.random.fold_in(stream_key, 3), *heavy), -limit, limit).astype(kind)


def setup_inputs(seed: int = 0) -> dict:
    splits = jax.random.split(jax.random.key(seed), 5)
    local_weight = bell_draw_with(splits[0], (WORKERS, FRAG, D), FRAG ** -0.5, 0.75, ((0, 64), (2, 16)), (0, 1, 64, 4.0))
    anchor = bell_draw(splits[1], (FRAG, D), FRAG ** -0.5, 0.25, ((1, 16),), jnp.float32)
    momentum = bell_draw(splits[2], (FRAG, D), 0.05, 0.3, ((0, 64), (1, 16)), jnp.float32)
    tokens = bell_draw(splits[3], (TOKENS, FRAG), 1.0, 6.0, ((0, 1024),))
    return dict(local_weight=local_weight, anchor=anchor, momentum=momentum, tokens=tokens)


outer_rate = 0.7
decay_rate = 0.9
blend_rate = 0.5


def reference(local_weight, anchor, momentum, tokens):
    pseudo = (anchor[None] - local_weight.astype(jnp.float32)).astype(jnp.bfloat16)
    pseudo = lax.optimization_barrier(pseudo)
    average = jnp.sum(pseudo.astype(jnp.float32), axis=0) / WORKERS
    momentum_out = decay_rate * momentum + average
    anchor_out = anchor - outer_rate * (average + decay_rate * momentum_out)
    blended = (blend_rate * anchor_out[None] + (1.0 - blend_rate) * local_weight.astype(jnp.float32)).astype(jnp.bfloat16)
    grouped = tokens.reshape(WORKERS, TOKENS // WORKERS, FRAG)

    def worker_product(pair):
        rows, weight = pair
        return jnp.dot(rows, weight, preferred_element_type=jnp.float32).astype(jnp.bfloat16)

    product_out = lax.map(worker_product, (grouped, blended)).reshape(TOKENS, D)
    return blended, anchor_out, momentum_out, product_out
```

```python
import functools

import jax
import jax.numpy as jnp
from jax import lax
from jax.experimental import pallas as pl
from jax.experimental.pallas import tpu as pltpu
from jax.sharding import Mesh, PartitionSpec as P


outer_rate = 0.7
decay_rate = 0.9
blend_rate = 0.5

Y, ZLO, CORE, ZHI, X = 4, 8, 2, 4, 4
HOP = 2
ring = ("zlo", "zhi")


def at_z(z):
    z %= ZHI * ZLO
    return z % ZLO * ZHI + z // ZLO


def shift(hop):
    return [(at_z(z), at_z(z + hop)) for z in range(ZHI * ZLO)]


def exchange(tiles, axis):
    return lax.all_to_all(tiles, axis, 0, 0, tiled=True)


def from_all(shard, axis):
    peers = lax.axis_size(axis)
    return exchange(jnp.broadcast_to(shard[None], (peers, *shard.shape)), axis)


def product_kernel(lengths, tokens_ref, *refs):
    pieces, out_ref = list(refs[:-1]), refs[-1]
    rows = out_ref.shape[2]
    for block, sizes in enumerate(lengths):
        total, first = None, 0
        for size in sizes:
            part = jnp.dot(
                tokens_ref[:, first : first + size],
                pieces.pop(0)[...],
                preferred_element_type=jnp.float32,
            )
            total = part if total is None else total + part
            first += size
        for x in range(X):
            out_ref[x, block] = total[x * rows : (x + 1) * rows].astype(jnp.bfloat16)


def product(tokens, blocks):
    rows, depth = tokens.shape
    columns = blocks[0][0].shape[1]
    lengths = tuple(tuple(p.shape[0] for p in pieces) for pieces in blocks)
    pieces = [p for pieces in blocks for p in pieces]
    return pl.pallas_call(
        functools.partial(product_kernel, lengths),
        out_shape=jax.ShapeDtypeStruct(
            (X, len(blocks), rows // X, columns), jnp.bfloat16
        ),
        in_specs=[pl.BlockSpec(memory_space=pltpu.VMEM)] * (1 + len(pieces)),
        out_specs=pl.BlockSpec(memory_space=pltpu.VMEM),
        compiler_params=pltpu.CompilerParams(vmem_limit_bytes=16 << 20),
        cost_estimate=pl.CostEstimate(
            flops=2 * rows * depth * columns * len(blocks),
            bytes_accessed=2 * (rows * depth + 2 * len(blocks) * depth * columns),
            transcendentals=0,
        ),
    )(tokens, *pieces)


def lay_out_kernel(blocks, zhi_ref, *refs):
    sources, out_ref, sems = refs[:-2], refs[-2], refs[-1]
    columns = sources[0].shape[3]
    copies = []
    for shift, source, block in blocks:
        at = lax.rem(zhi_ref[0] + shift, ZHI) * (X * columns)
        for x in range(X):
            place = pl.multiple_of(at + x * columns, columns)
            copies.append(
                pltpu.make_async_copy(
                    sources[source].at[x, block],
                    out_ref.at[:, pl.ds(place, columns)],
                    sems.at[shift, x],
                )
            )
    for copy in copies:
        copy.start()
    for copy in copies:
        copy.wait()


def lay_out(zhi, near, far):
    _, _, rows, columns = near.shape
    blocks = ((0, 0, 0), (1, 0, 1), (3, 0, 2), (2, 1, 0))
    return pl.pallas_call(
        functools.partial(lay_out_kernel, blocks),
        name="lay_out",
        out_shape=jax.ShapeDtypeStruct((rows, ZHI * X * columns), jnp.bfloat16),
        in_specs=[pl.BlockSpec(memory_space=pltpu.SMEM)]
        + [pl.BlockSpec(memory_space=pltpu.VMEM)] * 2,
        out_specs=pl.BlockSpec(memory_space=pl.ANY),
        scratch_shapes=[pltpu.SemaphoreType.DMA((ZHI, X))],
        compiler_params=pltpu.CompilerParams(vmem_limit_bytes=16 << 20),
    )(zhi, near, far)


def per_device(local_weight, anchor, momentum, tokens):
    own = local_weight[0]
    depth, columns = own.shape
    zhi = lax.axis_index("zhi")
    place = (lax.axis_index("y") * ZLO + lax.axis_index("zlo")) * CORE + lax.axis_index("core")
    rows = depth // (Y * ZLO * CORE)
    half = depth // 2

    gathered = from_all(tokens, "x").reshape(-1, depth)

    pseudo = (anchor - own.astype(jnp.float32)).astype(jnp.bfloat16)
    pseudo = pseudo.reshape(Y, ZLO, CORE, rows, columns).transpose(0, 2, 1, 3, 4)
    pseudo = lax.optimization_barrier(pseudo.reshape(Y * CORE, ZLO, rows, columns))
    part = exchange(pseudo, ("y", "core"))
    part = jnp.sum(part.astype(jnp.float32), axis=0)
    part = exchange(part, "zlo")
    average = jnp.sum(part, axis=0) / (Y * ZLO * CORE)
    mine = lax.dynamic_slice_in_dim(anchor, place * rows, rows, 0)
    momentum_out = decay_rate * momentum + average
    updated = mine - outer_rate * (average + decay_rate * momentum_out)
    updated = updated.astype(jnp.bfloat16)
    updated = from_all(updated, "zlo")
    updated = from_all(updated, ("y", "core"))
    updated = updated.reshape(Y, CORE, ZLO, rows, columns).transpose(0, 2, 1, 3, 4)
    anchor_out = updated.reshape(depth, columns).astype(jnp.float32)
    blended = (
        blend_rate * anchor_out + (1.0 - blend_rate) * own.astype(jnp.float32)
    ).astype(jnp.bfloat16)

    top, bottom = blended[:half], blended[half:]
    blocks = [top, bottom, bottom, top]
    for _ in range(ZLO // HOP):
        for at in range(4):
            way = HOP if at % 2 == 0 else -HOP
            blocks[at] = lax.ppermute(blocks[at], ring, shift(way))
    below_top, above_bottom, below_bottom, above_top = blocks
    far_top = lax.ppermute(below_top, ring, shift(ZLO))
    far_bottom = lax.ppermute(above_bottom, ring, shift(-ZLO))
    far = [far_top, far_bottom]

    blocks = ([top, bottom], [above_top, above_bottom], [below_top, below_bottom])
    near = exchange(product(gathered, blocks), "x")
    far = exchange(product(gathered, (far,)), "x")
    product_out = lay_out(zhi[None], near, far)
    return (blended[None], anchor_out, momentum_out, product_out)


def solution(mesh):
    fine = Mesh(
        mesh.devices.reshape(Y, ZLO, CORE, ZHI, X), ("y", "zlo", "core", "zhi", "x")
    )
    replica, fsdp = ("y", "zlo", "core"), ("zhi", "x")
    placed = (
        P(replica, None, fsdp),
        P(None, fsdp),
        P(replica, fsdp),
        P((*replica, *fsdp), None),
    )

    return jax.shard_map(
        per_device, mesh=fine, in_specs=placed, out_specs=placed, check_vma=False
    )
```
